32 devices in a mesh: rep: 4 (over x, core), tp: 8 (over z, y).
Axes of the slice: x: 2, y: 2, z: 4, core: 2. Of those that a mesh axis runs over, the one named last changes fastest.
Arguments:
- trainer_query: float32 [32, 256, 8192], P(('rep', 'tp')), may hold values from -6 to 6
- trainer_output: float32 [32, 8192, 256], P(('rep', 'tp')), may hold values from -6 to 6
- probes: bfloat16 [768, 8192], replicated, may hold values from -0.0625 to 0.0625
- shard_block: int32 [32], replicated, may hold values from 0 to 31, each once
- slice_owner: int32 [8], replicated, may hold values from 0 to 7, each once
Outputs:
- query_slices: bfloat16 [8, 8192, 1024], P('tp')
- output_slices: bfloat16 [8, 1024, 8192], P('tp')
- query_prints: float32 [8, 768, 1024], P('tp')
- output_prints: float32 [8, 1024, 768], P('tp')
The draws below stay inside these ranges and needn't reach their ends.
Inputs may be any that keep to these rules, and one draw needn't show every extreme that they name: `shard_block`: a permutation: each number once. `slice_owner`: a permutation: each number once.
All inputs are finite; a program needn't handle non-finite values.
Results may differ from the reference program's by a relative error of at most 0.0029.
Values may be sent and summed in bfloat16 or wider, within the bound.
No kernel may reach another device: no remote copies, remote signals or barrier semaphores. Data moves between devices by JAX's collectives and lax.ppermute only.
A program may use at most 192 MiB of HBM per device.

```python
import jax
import jax.numpy as jnp

D = 8192
PROBES = 768
HQ = 8192
SHARD = 256
SLICE = 1024
N_TP = 8
DEVICES = 32


def shard_levels(rng, extent, shards, low, high):
    loudness = 1.0
    for dim, blocks in shards:
        heights = jax.random.uniform(jax.random.fold_in(jax.random.fold_in(rng, 6), dim), (blocks,), jnp.float32, low / len(shards), high / len(shards))
        loudness = loudness * jnp.repeat(jnp.exp(heights), extent[dim] // blocks).reshape((-1,) + (1,) * (len(extent) - 1 - dim))
    return loudness


def noise(stream_key, shape, deviation, reach, shards=(), kind=jnp.bfloat16):
    entries = deviation * jax.random.normal(stream_key, shape, jnp.float32)
    if shards:
        entries = entries * shard_levels(stream_key, shape, shards, -0.22, 0.18)
    return jnp.clip(entries, -reach, reach).astype(kind)


def setup_inputs(seed: int = 0) -> dict:
    streams_of = jax.random.split(jax.random.key(seed), 6)
    return {
        "trainer_query": noise(streams_of[0], (DEVICES, SHARD, HQ), 1.0, 6.0, ((0, 32),), jnp.float32),
        "trainer_output": noise(streams_of[1], (DEVICES, HQ, SHARD), 1.0, 6.0, ((0, 32),), jnp.float32),
        "probes": noise(streams_of[2], (PROBES, D), D ** -0.5, 0.0625),
        "shard_block": jax.random.permutation(streams_of[3], DEVICES).astype(jnp.int32),
        "slice_owner": jax.random.permutation(streams_of[4], N_TP).astype(jnp.int32),
    }


def reference(trainer_query, trainer_output, probes, shard_block, slice_owner):
    positions = jnp.arange(DEVICES, dtype=jnp.int32)
    inverse = jnp.zeros((DEVICES,), jnp.int32).at[shard_block].set(positions)
    query_full = trainer_query.astype(jnp.bfloat16)[inverse].reshape(D, HQ)
    output_full = jnp.transpose(trainer_output.astype(jnp.bfloat16)[inverse], (1, 0, 2)).reshape(HQ, D)
    query_slices = jnp.transpose(query_full.reshape(D, N_TP, SLICE)[:, slice_owner], (1, 0, 2))
    output_slices = output_full.reshape(N_TP, SLICE, D)[slice_owner]
    probe_wide = probes.astype(jnp.float32)
    query_prints = jnp.einsum("pd,jdc->jpc", probe_wide, query_slices.astype(jnp.float32))
    output_prints = jnp.einsum("jcd,pd->jcp", output_slices.astype(jnp.float32), probe_wide)
    return (query_slices, output_slices, query_prints, output_prints)
```

```python
import functools

import jax
import jax.numpy as jnp
from jax import lax
from jax.experimental import pallas as pl
from jax.experimental.pallas import tpu as pltpu
from jax.sharding import PartitionSpec as P


LANES = 128
TILE = 256
ROWS = 64
HBM = pl.BlockSpec(memory_space=pl.ANY)
SMEM = pl.BlockSpec(memory_space=pltpu.SMEM)


def tp_swap(value, offset):
    reps, tps = lax.axis_size("rep"), lax.axis_size("tp")
    pairs = [(r * tps + t, r * tps + (t ^ offset)) for r in range(reps) for t in range(tps)]
    return lax.ppermute(value, ("rep", "tp"), pairs)


def rep_swap(value, mask):
    reps, tps = lax.axis_size("rep"), lax.axis_size("tp")
    pairs = [(r * tps + t, (r ^ mask) * tps + t) for r in range(reps) for t in range(tps)]
    return lax.ppermute(value, ("rep", "tp"), pairs)


def cast_blocks(trainer_query, trainer_output, slice_owner, offsets, width):
    rows = trainer_query.shape[1]
    groups = width // rows
    count = len(offsets)

    def body(owner, query, output, *rest):
        outs, (query_in, output_in, packed, in_sems, out_sems) = rest[:count], rest[count:]
        me = lax.axis_index("tp")
        reads = []
        for i, offset in enumerate(offsets):
            start = pl.multiple_of(owner[me ^ offset] * width, width)
            reads.append((
                pltpu.make_async_copy(query.at[0, :, pl.ds(start, width)], query_in.at[i], in_sems.at[2 * i]),
                pltpu.make_async_copy(output.at[0, pl.ds(start, width), :], output_in.at[i], in_sems.at[2 * i + 1]),
            ))
            for read in reads[-1]:
                read.start()
        writes = []
        for i in range(count):
            reads[i][0].wait()

            def query_step(k, carry, i=i):
                at = pl.ds(pl.multiple_of(k * ROWS, ROWS), ROWS)
                packed[i, at, :] = query_in[i, at, :].astype(jnp.bfloat16)
                return carry

            lax.fori_loop(0, rows // ROWS, query_step, 0)
            reads[i][1].wait()
            for g in range(groups):

                def output_step(k, carry, i=i, g=g):
                    base = pl.multiple_of(k * ROWS, ROWS)
                    packed[i, pl.ds(rows + base, ROWS), g * rows:(g + 1) * rows] = (
                        output_in[i, pl.ds(g * rows + base, ROWS), :].astype(jnp.bfloat16)
                    )
                    return carry

                lax.fori_loop(0, rows // ROWS, output_step, 0)
            writes.append(pltpu.make_async_copy(packed.at[i], outs[i], out_sems.at[i]))
            writes[-1].start()
        for write in writes:
            write.wait()

    return pl.pallas_call(
        body,
        out_shape=[jax.ShapeDtypeStruct((2 * rows, width), jnp.bfloat16)] * count,
        in_specs=[SMEM, HBM, HBM],
        out_specs=[HBM] * count,
        scratch_shapes=[
            pltpu.VMEM((count, rows, width), jnp.float32),
            pltpu.VMEM((count, width, rows), jnp.float32),
            pltpu.VMEM((count, 2 * rows, width), jnp.bfloat16),
            pltpu.SemaphoreType.DMA((2 * count,)),
            pltpu.SemaphoreType.DMA((count,)),
        ],
        name="cast_blocks",
    )(slice_owner, trainer_query, trainer_output)


def absorb(state, blocks, probes, shard_block, rows, width):
    tps = lax.axis_size("tp")
    devices = tps * lax.axis_size("rep")
    count = len(blocks)
    groups = width // rows
    model = rows * devices
    prints = probes.shape[0]
    first = state is None
    depth = count * rows

    def body(places, probe, *rest):
        arrays, rest = rest[:count], rest[count:]
        if not first:
            rest = rest[2:] if False else rest[4:]
        (query_out, output_out, query_acc, output_acc), rest = rest[:4], rest[4:]
        query_buf, output_buf, probe_buf, query_sum, output_sum, in_sems, out_sems, acc_sems = rest
        me, rep = lax.axis_index("tp"), lax.axis_index("rep")
        starts = [
            pl.multiple_of(places[(rep ^ mask) * tps + (me ^ offset)] * rows, rows)
            for offset, mask, _ in blocks
        ]
        spans = [slice(i * rows, (i + 1) * rows) for i in range(count)]
        loads = []
        if not first:
            loads = [
                pltpu.make_async_copy(query_acc, query_sum, acc_sems.at[0]),
                pltpu.make_async_copy(output_acc, output_sum, acc_sems.at[1]),
            ]
        query_reads, output_reads, probe_reads = [], [], []
        per = 2 + groups
        for i in range(count):
            probe_reads.append(pltpu.make_async_copy(
                probe.at[:, pl.ds(starts[i], rows)], probe_buf.at[:, spans[i]], in_sems.at[per * i]))
            query_reads.append(pltpu.make_async_copy(
                arrays[i].at[0:rows, :], query_buf.at[spans[i], :], in_sems.at[per * i + 1]))
            output_reads.append([
                pltpu.make_async_copy(
                    arrays[i].at[rows:2 * rows, g * rows:(g + 1) * rows],
                    output_buf.at[g * rows:(g + 1) * rows, spans[i]], in_sems.at[per * i + 2 + g])
                for g in range(groups)
            ])
        for copy in query_reads + probe_reads + loads[:1]:
            copy.start()
        for copies in output_reads:
            for copy in copies:
                copy.start()
        for copy in loads[1:]:
            copy.start()
        writes = []
        for i in range(count):
            query_reads[i].wait()
            writes.append(pltpu.make_async_copy(
                query_buf.at[spans[i], :], query_out.at[pl.ds(starts[i], rows), :], out_sems.at[i]))
            writes[-1].start()
        for copy in probe_reads + loads[:1]:
            copy.wait()

        def query_step(n, carry):
            at = pl.ds(pl.multiple_of(n * TILE, TILE), TILE)
            part = jnp.dot(probe_buf[...], query_buf[:, at], preferred_element_type=jnp.float32)
            query_sum[:, at] = part if first else query_sum[:, at] + part
            return carry

        lax.fori_loop(0, width // TILE, query_step, 0)
        stores = [pltpu.make_async_copy(query_sum, query_acc, acc_sems.at[2])]
        stores[0].start()
        for i in range(count):
            for copy in output_reads[i]:
                copy.wait()
            writes.append(pltpu.make_async_copy(
                output_buf.at[:, spans[i]], output_out.at[:, pl.ds(starts[i], rows)], out_sems.at[count + i]))
            writes[-1].start()
        for copy in loads[1:]:
            copy.wait()

        def output_step(n, carry):
            at = pl.ds(pl.multiple_of(n * TILE, TILE), TILE)
            part = lax.dot_general(
                output_buf[at, :], probe_buf[...], (((1,), (1,)), ((), ())), preferred_element_type=jnp.float32)
            output_sum[at, :] = part if first else output_sum[at, :] + part
            return carry

        lax.fori_loop(0, width // TILE, output_step, 0)
        stores.append(pltpu.make_async_copy(output_sum, output_acc, acc_sems.at[3]))
        stores[1].start()
        for copy in writes + stores:
            copy.wait()

    shapes = [
        jax.ShapeDtypeStruct((model, width), jnp.bfloat16),
        jax.ShapeDtypeStruct((width, model), jnp.bfloat16),
        jax.ShapeDtypeStruct((prints, width), jnp.float32),
        jax.ShapeDtypeStruct((width, prints), jnp.float32),
    ]
    held = [] if first else list(state)
    return pl.pallas_call(
        body,
        out_shape=shapes,
        in_specs=[SMEM, HBM] + [HBM] * (count + len(held)),
        out_specs=[HBM] * 4,
        input_output_aliases={} if first else {2 + count + i: i for i in range(4)},
        scratch_shapes=[
            pltpu.VMEM((depth, width), jnp.bfloat16),
            pltpu.VMEM((width, depth), jnp.bfloat16),
            pltpu.VMEM((prints, depth), jnp.bfloat16),
            pltpu.VMEM((prints, width), jnp.float32),
            pltpu.VMEM((width, prints), jnp.float32),
            pltpu.SemaphoreType.DMA(((2 + groups) * count,)),
            pltpu.SemaphoreType.DMA((2 * count,)),
            pltpu.SemaphoreType.DMA((4,)),
        ],
        cost_estimate=pl.CostEstimate(
            flops=4 * prints * width * depth, bytes_accessed=12 * depth * width + 16 * prints * width, transcendentals=0),
        name="absorb",
    )(shard_block, probes, *[array for _, _, array in blocks], *held)


def spread(sent, offset):
    reps = lax.axis_size("rep")
    near = tp_swap(sent, offset) if offset else sent
    found = []
    for mask in range(0, reps, 2):
        block = rep_swap(near, mask) if mask else near
        found.append((mask, block))
        if mask + 1 < reps:
            found.append((mask + 1, rep_swap(block, 1)))
    return found


def whole_blocks(trainer_query, trainer_output, probes, shard_block, slice_owner):
    tps, reps = lax.axis_size("tp"), lax.axis_size("rep")
    me, rep = lax.axis_index("tp"), lax.axis_index("rep")
    rows, width = trainer_query.shape[1], trainer_query.shape[2] // tps
    query_local = trainer_query[0].astype(jnp.bfloat16)
    output_local = trainer_output[0].astype(jnp.bfloat16)
    query_parts, output_parts, sources = [], [], []
    for offset in range(tps):
        start = slice_owner[me ^ offset] * width
        query_sent = lax.dynamic_slice(query_local, (0, start), (rows, width))
        output_sent = lax.dynamic_slice(output_local, (start, 0), (width, rows))
        for mask, block in spread(query_sent, offset):
            query_parts.append(block)
            sources.append((rep ^ mask) * tps + (me ^ offset))
        output_parts += [block for _, block in spread(output_sent, offset)]
    devices = tps * reps
    places = jnp.take(shard_block, jnp.stack(sources))
    order = jnp.zeros((devices,), jnp.int32).at[places].set(jnp.arange(devices, dtype=jnp.int32))
    query_slice = jnp.take(jnp.stack(query_parts), order, axis=0).reshape(rows * devices, width)
    output_slice = jnp.take(jnp.stack(output_parts, axis=1), order, axis=1).reshape(width, rows * devices)
    query_prints = jnp.dot(probes, query_slice, preferred_element_type=jnp.float32)
    output_prints = lax.dot_general(
        output_slice, probes, (((1,), (1,)), ((), ())), preferred_element_type=jnp.float32
    )
    return query_slice, output_slice, query_prints, output_prints


def per_device(trainer_query, trainer_output, probes, shard_block, slice_owner):
    tps = lax.axis_size("tp")
    rows, width = trainer_query.shape[1], trainer_query.shape[2] // tps
    if rows % LANES or width % rows or width % TILE:
        results = whole_blocks(trainer_query, trainer_output, probes, shard_block, slice_owner)
    else:
        half = tps // 2
        sent = []
        for part in (range(half), range(half, tps)):
            sent += cast_blocks(trainer_query, trainer_output, slice_owner, tuple(part), width)
        found = [spread(sent[offset], offset) for offset in range(tps)]
        results = None
        for offset in range(tps):
            blocks = [(offset, mask, block) for mask, block in found[offset]]
            results = absorb(results, blocks, probes, shard_block, rows, width)
    return tuple(value[None] for value in results)


def solution(mesh):
    placed = (P(("rep", "tp"), None, None), P(("rep", "tp"), None, None), P(), P(), P())
    return jax.shard_map(
        per_device,
        mesh=mesh,
        in_specs=placed,
        out_specs=(
            P("tp", None, None),
            P("tp", None, None),
            P("tp", None, None),
            P("tp", None, None),
        ),
        check_vma=False,
    )
```
